32 devices in a mesh: img: 8 (over z, x), row: 4 (over y, core).
Axes of the slice: x: 2, y: 2, z: 4, core: 2. Of those that a mesh axis runs over, the one named last changes fastest.
Arguments:
- tokens: bfloat16 [8, 32, 128, 1024], P('img', 'row'), may hold values from -14 to 14
- proj_weight: bfloat16 [1024, 256], replicated, may hold values from -0.1875 to 0.1875
- proj_bias: float32 [256], replicated, may hold values from -3 to 3
- conv_weight: bfloat16 [4, 3, 3, 256, 256], replicated, may hold values from -0.125 to 0.125
- bn_gain: float32 [4, 256], replicated, may hold values from 0.1 to 1.9
- bn_bias: float32 [4, 256], replicated, may hold values from -3 to 3
Outputs:
- joining_out: bfloat16 [8, 32, 128, 256], P('img', 'row')
The draws below stay inside these ranges and needn't reach their ends.
All inputs are finite; a program needn't handle non-finite values.
Results may differ from the reference program's by a relative error of at most 0.0071.
Values may be sent and summed in bfloat16 or wider, within the bound.
A program may use at most 64 MiB of HBM per device.

```python
import math
import jax
import jax.numpy as jnp
from jax import lax

EMBED = 1024
FW = 256
COLS = 128
IMAGES = 8
HEIGHT = 32


def draw_tokens(key, part):
    key_image, key_row, key_base = jax.random.split(key, 3)
    image_scale = jnp.exp(jax.random.uniform(key_image, (IMAGES, 1, 1, 1), jnp.float32, 0.0, math.log(4.0)))
    row_scale = jnp.exp(jax.random.uniform(key_row, (1, HEIGHT, 1, 1), jnp.float32, 0.0, math.log(2.5)))
    base = jnp.clip(jax.random.normal(key_base, (IMAGES, HEIGHT, COLS, EMBED), jnp.float32), -4.0, 4.0)
    return (base * image_scale * row_scale / 3.0).astype(jnp.bfloat16)


def centred(key, dims, deviation, most, kind=jnp.bfloat16):
    return jnp.clip(deviation * jax.random.normal(key, dims, jnp.float32), -most, most).astype(kind)


def setup_inputs(seed: int = 0) -> dict:
    key_of = jax.random.split(jax.random.key(seed), 7)
    tokens = draw_tokens(jax.random.fold_in(key_of[6], 71), 0)
    proj_weight = centred(key_of[1], (EMBED, FW), EMBED ** -0.5, 0.1875)
    proj_bias = centred(key_of[2], (FW,), 0.5, 3.0, jnp.float32)
    conv_weight = centred(key_of[3], (4, 3, 3, FW, FW), (9 * FW) ** -0.5, 0.125)
    bn_gain = jnp.clip(1.0 + 0.18 * jax.random.normal(key_of[4], (4, FW), jnp.float32), 0.1, 1.9)
    bn_bias = centred(key_of[5], (4, FW), 0.5, 3.0, jnp.float32)
    return {"tokens": tokens, "proj_weight": proj_weight, "proj_bias": proj_bias, "conv_weight": conv_weight, "bn_gain": bn_gain, "bn_bias": bn_bias}


epsilon = 1e-05

def conv_three(source, kernel):
    return lax.conv_general_dilated(source.astype(jnp.float32), kernel.astype(jnp.float32), (1, 1), ((1, 1), (1, 1)), dimension_numbers=('NHWC', 'HWIO', 'NHWC'), precision=lax.Precision.HIGHEST)

def batch_norm(conv_out, gain_row, shift_row):
    average = lax.optimization_barrier(jnp.mean(conv_out, axis=(0, 1, 2)))
    spread = lax.optimization_barrier(jnp.mean(jnp.square(conv_out - average), axis=(0, 1, 2)))
    return (conv_out - average) * lax.rsqrt(spread + epsilon) * gain_row + shift_row

def residual_unit(source, conv_weight, bn_gain, bn_bias, first):
    active = jax.nn.relu(source)
    conv_first = conv_three(active, conv_weight[first])
    hidden = jax.nn.relu(batch_norm(conv_first, bn_gain[first], bn_bias[first])).astype(jnp.bfloat16)
    conv_second = conv_three(hidden, conv_weight[first + 1])
    return source.astype(jnp.float32) + batch_norm(conv_second, bn_gain[first + 1], bn_bias[first + 1])

def reference(tokens, proj_weight, proj_bias, conv_weight, bn_gain, bn_bias):
    img_count, row_count, col_count, embed_dim = tokens.shape
    flat = jnp.dot(tokens.reshape(-1, embed_dim), proj_weight, preferred_element_type=jnp.float32) + proj_bias
    feature = flat.astype(jnp.bfloat16).reshape(img_count, row_count, col_count, -1)
    joined = residual_unit(feature, conv_weight, bn_gain, bn_bias, 0).astype(jnp.bfloat16)
    return residual_unit(joined, conv_weight, bn_gain, bn_bias, 2).astype(jnp.bfloat16)
```

```python
import functools

import jax
import jax.numpy as jnp
from jax import lax
from jax.experimental import pallas as pl
from jax.experimental.pallas import tpu as pltpu
from jax.sharding import PartitionSpec as P

epsilon = 1e-05
MESH = pl.DeviceIdType.MESH
F32 = jnp.float32
BF16 = jnp.bfloat16


def kernel(
    imgs,
    strips,
    height,
    cols,
    tokens_ref,
    pw_ref,
    pb_ref,
    cw_ref,
    gain_ref,
    bias_ref,
    out_ref,
    tok,
    pw,
    cw,
    feat,
    joined,
    xcat,
    raw,
    stat,
    peers,
    load_sem,
    weight_sem,
    halo_send,
    halo_recv,
    stat_send,
    stat_recv,
):
    count = imgs * strips
    width = feat.shape[-1]
    cells = height * cols
    me_img, me_row = lax.axis_index("img"), lax.axis_index("row")
    me = me_img * strips + me_row
    has_up, has_down = me_row > 0, me_row < strips - 1

    def peer(distance):
        target = lax.rem(me + distance, count)
        return {"img": target // strips, "row": lax.rem(target, strips)}

    def rows(first, number):
        return pl.ds(first * cols, number * cols)

    loads = [
        pltpu.make_async_copy(pw_ref, pw, load_sem.at[0]),
        pltpu.make_async_copy(tokens_ref.at[rows(0, 1)], tok.at[rows(0, 1)], load_sem.at[1]),
        pltpu.make_async_copy(
            tokens_ref.at[rows(height - 1, 1)], tok.at[rows(height - 1, 1)], load_sem.at[2]
        ),
        pltpu.make_async_copy(
            tokens_ref.at[rows(1, height - 2)], tok.at[rows(1, height - 2)], load_sem.at[3]
        ),
    ]
    weights = [
        pltpu.make_async_copy(
            cw_ref.at[pl.ds(3 * k, 3)], cw.at[pl.ds(3 * k, 3)], weight_sem.at[k]
        )
        for k in range(4)
    ]
    for load in loads:
        load.start()
    weights[0].start()

    barrier = pltpu.get_barrier_semaphore()

    @pl.loop(1, count)
    def _(distance):
        pl.semaphore_signal(barrier, inc=1, device_id=peer(distance), device_id_type=MESH)

    for k in range(1, 4):
        weights[k].start()

    @pl.when(jnp.logical_not(has_up))
    def _():
        xcat[rows(0, 1), :] = jnp.zeros((cols, 3 * width), BF16)

    @pl.when(jnp.logical_not(has_down))
    def _():
        xcat[rows(height + 1, 1), :] = jnp.zeros((cols, 3 * width), BF16)

    column = lax.broadcasted_iota(jnp.int32, (cols, width), 0)

    def span(row):
        return pl.ds(pl.multiple_of(row * cols, cols), cols)

    def put(row, value):
        at = span(row)
        xcat[at, 0:width] = jnp.where(column == 0, 0.0, pltpu.roll(value, 1, 0)).astype(BF16)
        xcat[at, width : 2 * width] = value.astype(BF16)
        xcat[at, 2 * width : 3 * width] = jnp.where(
            column == cols - 1, 0.0, pltpu.roll(value, cols - 1, 0)
        ).astype(BF16)

    def project(row):
        value = jnp.dot(tok[span(row), :], pw[...], preferred_element_type=F32) + pb_ref[...]
        value = value.astype(BF16)
        feat[span(row + 1), :] = value
        put(row + 1, jnp.maximum(value.astype(F32), 0.0))

    def halo(ref, phase):
        up = pltpu.make_async_remote_copy(
            src_ref=ref.at[rows(1, 1)],
            dst_ref=ref.at[rows(height + 1, 1)],
            send_sem=halo_send.at[phase, 0],
            recv_sem=halo_recv.at[phase, 1],
            device_id={"img": me_img, "row": jnp.maximum(me_row - 1, 0)},
            device_id_type=MESH,
        )
        down = pltpu.make_async_remote_copy(
            src_ref=ref.at[rows(height, 1)],
            dst_ref=ref.at[rows(0, 1)],
            send_sem=halo_send.at[phase, 1],
            recv_sem=halo_recv.at[phase, 0],
            device_id={"img": me_img, "row": jnp.minimum(me_row + 1, strips - 1)},
            device_id_type=MESH,
        )
        return up, down

    def send_halo(ref, phase):
        up, down = halo(ref, phase)

        @pl.when(has_up)
        def _():
            up.start()

        @pl.when(has_down)
        def _():
            down.start()

    def take_halo(ref, phase, top, bottom):
        up, down = halo(ref, phase)

        @pl.when(has_up)
        def _():
            down.wait_recv()
            top()

        @pl.when(has_down)
        def _():
            up.wait_recv()
            bottom()

    def end_halo(ref, phase):
        up, down = halo(ref, phase)

        @pl.when(has_up)
        def _():
            up.wait_send()

        @pl.when(has_down)
        def _():
            down.wait_send()

    def conv(k, first, number):
        total = None
        for dy in range(3):
            part = jnp.dot(
                xcat[rows(first + dy, number), :], cw[3 * k + dy], preferred_element_type=F32
            )
            total = part if total is None else total + part
        raw[k, rows(first + 1, number), :] = total
        return jnp.sum(total, axis=0, keepdims=True)

    def stat_copy(k, distance):
        return pltpu.make_async_remote_copy(
            src_ref=stat.at[k],
            dst_ref=peers.at[k, distance - 1],
            send_sem=stat_send.at[k],
            recv_sem=stat_recv.at[k],
            device_id=peer(distance),
            device_id_type=MESH,
        )

    def send_stat(k, sums):
        centre = sums / cells

        def add_row(row, squares):
            return squares + jnp.sum(
                jnp.square(raw[k, span(row + 1), :] - centre), axis=0, keepdims=True
            )

        squares = lax.fori_loop(0, height, add_row, jnp.zeros((1, width), F32))
        stat[k] = jnp.concatenate([sums, squares], axis=0)

        @pl.loop(1, count)
        def _(distance):
            stat_copy(k, distance).start()

    def take_stat(k):
        pltpu.make_async_copy(peers.at[k], peers.at[k], stat_recv.at[k]).wait()
        own = stat[k]
        every = peers[k]
        total = jnp.sum(every, axis=0) + own
        average = total[0:1] / (count * cells)
        gaps = jnp.sum(jnp.square(every[:, 0, :] - cells * average), axis=0, keepdims=True)
        gaps += jnp.square(own[0:1] - cells * average)
        spread = (total[1:2] + gaps / cells) / (count * cells)
        scale = lax.rsqrt(spread + epsilon) * gain_ref[pl.ds(k, 1), :]
        return average, scale, bias_ref[pl.ds(k, 1), :]

    def normed(k, row, norm):
        average, scale, shift = norm
        return (raw[k, span(row), :] - average) * scale + shift

    rim_first = [(0, 2), (height - 2, 2)]
    middle = [(first, 2) for first in range(2, height - 2, 2)]

    loads[0].wait()
    loads[1].wait()
    project(0)
    loads[2].wait()
    project(height - 1)
    pl.semaphore_wait(barrier, count - 1)
    send_halo(feat, 0)
    loads[3].wait()

    @pl.loop(1, height - 1)
    def _(row):
        project(row)

    def feature_rim(row):
        put(row, jnp.maximum(feat[span(row), :].astype(F32), 0.0))

    weights[0].wait()
    sums = sum(conv(0, first, number) for first, number in middle)
    take_halo(feat, 0, lambda: feature_rim(0), lambda: feature_rim(height + 1))
    sums += sum(conv(0, first, number) for first, number in rim_first)
    send_halo(raw.at[0], 1)
    send_stat(0, sums)

    def later_conv(k):
        weights[k].wait()
        sums = sum(conv(k, first, number) for first, number in rim_first)
        if k < 3:
            send_halo(raw.at[k], k + 1)
        sums += sum(conv(k, first, number) for first, number in middle)
        send_stat(k, sums)

    def hidden(k):
        norm = take_stat(k)

        def one(row):
            put(row, jnp.maximum(normed(k, row, norm), 0.0))

        pl.loop(1, height + 1)(one)
        take_halo(raw.at[k], k + 1, lambda: one(0), lambda: one(height + 1))

    hidden(0)
    later_conv(1)

    norm_1 = take_stat(1)

    def join(row, local):
        value = (feat[span(row), :].astype(F32) + normed(1, row, norm_1)).astype(BF16)
        if local:
            joined[span(row - 1), :] = value
        put(row, jnp.maximum(value.astype(F32), 0.0))

    pl.loop(1, height + 1)(lambda row: join(row, True))
    take_halo(raw.at[1], 2, lambda: join(0, False), lambda: join(height + 1, False))
    later_conv(2)
    hidden(2)
    later_conv(3)
    norm_3 = take_stat(3)

    @pl.loop(0, height)
    def _(row):
        value = joined[span(row), :].astype(F32) + normed(3, row + 1, norm_3)
        out_ref[span(row), :] = value.astype(BF16)

    end_halo(feat, 0)
    for k in range(3):
        end_halo(raw.at[k], k + 1)
    for k in range(4):
        pltpu.make_async_copy(peers.at[k], peers.at[k], stat_send.at[k]).wait()


def solution(mesh):
    imgs, strips = mesh.shape["img"], mesh.shape["row"]

    def on_device(tokens, proj_weight, proj_bias, conv_weight, bn_gain, bn_bias):
        images, height, cols, embed = tokens.shape
        convs, taps, _, width, _ = conv_weight.shape
        assert images == 1 and height % 2 == 0 and height >= 4
        count = imgs * strips
        cells = height * cols
        any_space = pl.BlockSpec(memory_space=pl.ANY)
        vmem = pl.BlockSpec(memory_space=pltpu.VMEM)
        out = pl.pallas_call(
            functools.partial(kernel, imgs, strips, height, cols),
            out_shape=jax.ShapeDtypeStruct((cells, width), BF16),
            in_specs=[any_space, any_space, vmem, any_space, vmem, vmem],
            out_specs=vmem,
            scratch_shapes=[
                pltpu.VMEM((cells, embed), BF16),
                pltpu.VMEM((embed, width), BF16),
                pltpu.VMEM((convs * taps, taps * width, width), BF16),
                pltpu.VMEM((cells + 2 * cols, width), BF16),
                pltpu.VMEM((cells, width), BF16),
                pltpu.VMEM((cells + 2 * cols, taps * width), BF16),
                pltpu.VMEM((convs, cells + 2 * cols, width), F32),
                pltpu.VMEM((convs, 2, width), F32),
                pltpu.VMEM((convs, count - 1, 2, width), F32),
                pltpu.SemaphoreType.DMA((4,)),
                pltpu.SemaphoreType.DMA((convs,)),
                pltpu.SemaphoreType.DMA((convs, 2)),
                pltpu.SemaphoreType.DMA((convs, 2)),
                pltpu.SemaphoreType.DMA((convs,)),
                pltpu.SemaphoreType.DMA((convs,)),
            ],
            compiler_params=pltpu.CompilerParams(
                collective_id=0, has_side_effects=True, vmem_limit_bytes=48 * 1024 * 1024
            ),
        )(
            tokens.reshape(cells, embed),
            proj_weight,
            proj_bias.reshape(1, width),
            conv_weight.reshape(convs * taps, taps * width, width),
            bn_gain,
            bn_bias,
        )
        return out.reshape(images, height, cols, width)

    in_specs = (P("img", "row", None, None), P(), P(), P(), P(), P())
    return jax.shard_map(
        on_device,
        mesh=mesh,
        in_specs=in_specs,
        out_specs=P("img", "row", None, None),
        check_vma=False,
    )
```

```python
import functools

import jax
import jax.numpy as jnp
from jax import lax
from jax.experimental import pallas as pl
from jax.experimental.pallas import tpu as pltpu
from jax.sharding import PartitionSpec as P

epsilon = 1e-05
MESH = pl.DeviceIdType.MESH
F32 = jnp.float32
BF16 = jnp.bfloat16
PLAN = ("flat",)
UNROLL = 0
ROWS = 2
VMEM_LIMIT = 62 * 1024 * 1024


def kernel(
    imgs,
    strips,
    height,
    cols,
    tokens_ref,
    pw_ref,
    pb_ref,
    cw_ref,
    gain_ref,
    bias_ref,
    out_ref,
    tok,
    pw,
    cw,
    feat,
    joined,
    xcat,
    raw,
    stats,
    peers,
    load_sem,
    weight_sem,
    halo_send,
    halo_recv,
    stat_send,
    stat_recv,
):
    count = imgs * strips
    width = feat.shape[-1]
    cells = height * cols
    me_img, me_row = lax.axis_index("img"), lax.axis_index("row")
    me = me_img * strips + me_row
    has_up, has_down = me_row > 0, me_row < strips - 1

    def peer(distance):
        target = lax.rem(me + distance, count)
        return {"img": target // strips, "row": lax.rem(target, strips)}

    def row_peer(distance):
        return {"img": me_img, "row": lax.rem(me_row + distance, strips)}

    def img_peer(distance):
        return {"img": lax.rem(me_img + distance, imgs), "row": me_row}

    def core_peer(distance):
        return {"img": me_img, "row": me_row + 1 - 2 * lax.rem(me_row, 2)}

    def chip_peer(distance):
        chips = strips // 2
        target = lax.rem(me_img * chips + me_row // 2 + distance, imgs * chips)
        return {"img": target // chips, "row": 2 * lax.rem(target, chips) + lax.rem(me_row, 2)}

    peer_of = {
        "flat": peer, "row": row_peer, "img": img_peer, "core": core_peer, "chip": chip_peer
    }

    def rows(first, number):
        return pl.ds(first * cols, number * cols)

    loads = [
        pltpu.make_async_copy(pw_ref, pw, load_sem.at[0]),
        pltpu.make_async_copy(tokens_ref.at[rows(0, 1)], tok.at[rows(0, 1)], load_sem.at[1]),
        pltpu.make_async_copy(
            tokens_ref.at[rows(height - 1, 1)], tok.at[rows(height - 1, 1)], load_sem.at[2]
        ),
        pltpu.make_async_copy(
            tokens_ref.at[rows(1, height - 2)], tok.at[rows(1, height - 2)], load_sem.at[3]
        ),
    ]
    weights = [
        pltpu.make_async_copy(
            cw_ref.at[pl.ds(3 * k, 3)], cw.at[pl.ds(3 * k, 3)], weight_sem.at[k]
        )
        for k in range(4)
    ]
    for load in loads:
        load.start()
    weights[0].start()

    barrier = pltpu.get_barrier_semaphore()

    @pl.loop(1, count)
    def _(distance):
        pl.semaphore_signal(barrier, inc=1, device_id=peer(distance), device_id_type=MESH)

    for k in range(1, 4):
        weights[k].start()

    @pl.when(jnp.logical_not(has_up))
    def _():
        xcat[rows(0, 1), :] = jnp.zeros((cols, 3 * width), BF16)

    @pl.when(jnp.logical_not(has_down))
    def _():
        xcat[rows(height + 1, 1), :] = jnp.zeros((cols, 3 * width), BF16)

    column = lax.broadcasted_iota(jnp.int32, (cols, width), 0)

    def span(row):
        return pl.ds(pl.multiple_of(row * cols, cols), cols)

    def put(row, value):
        at = span(row)
        xcat[at, 0:width] = jnp.where(column == 0, 0.0, pltpu.roll(value, 1, 0)).astype(BF16)
        xcat[at, width : 2 * width] = value.astype(BF16)
        xcat[at, 2 * width : 3 * width] = jnp.where(
            column == cols - 1, 0.0, pltpu.roll(value, cols - 1, 0)
        ).astype(BF16)

    def project(row):
        value = jnp.dot(tok[span(row), :], pw[...], preferred_element_type=F32) + pb_ref[...]
        value = value.astype(BF16)
        feat[span(row + 1), :] = value
        put(row + 1, jnp.maximum(value.astype(F32), 0.0))

    def halo(ref, phase):
        up = pltpu.make_async_remote_copy(
            src_ref=ref.at[rows(1, 1)],
            dst_ref=ref.at[rows(height + 1, 1)],
            send_sem=halo_send.at[phase, 0],
            recv_sem=halo_recv.at[phase, 1],
            device_id={"img": me_img, "row": jnp.maximum(me_row - 1, 0)},
            device_id_type=MESH,
        )
        down = pltpu.make_async_remote_copy(
            src_ref=ref.at[rows(height, 1)],
            dst_ref=ref.at[rows(0, 1)],
            send_sem=halo_send.at[phase, 1],
            recv_sem=halo_recv.at[phase, 0],
            device_id={"img": me_img, "row": jnp.minimum(me_row + 1, strips - 1)},
            device_id_type=MESH,
        )
        return up, down

    def send_halo(ref, phase):
        up, down = halo(ref, phase)

        @pl.when(has_up)
        def _():
            up.start()

        @pl.when(has_down)
        def _():
            down.start()

    def take_halo(ref, phase, top, bottom):
        up, down = halo(ref, phase)

        @pl.when(has_up)
        def _():
            down.wait_recv()
            top()

        @pl.when(has_down)
        def _():
            up.wait_recv()
            bottom()

    def end_halo(ref, phase):
        up, down = halo(ref, phase)

        @pl.when(has_up)
        def _():
            up.wait_send()

        @pl.when(has_down)
        def _():
            down.wait_send()

    def taps(k, first, number, which):
        return sum(
            jnp.dot(xcat[rows(first + dy, number), :], cw[3 * k + dy], preferred_element_type=F32)
            for dy in which
        )

    def moments(value):
        size = value.shape[0]
        first = jnp.sum(value, axis=0, keepdims=True)
        squares = jnp.sum(jnp.square(value - first / size), axis=0, keepdims=True)
        return first, squares, size

    def conv(k, first, number):
        value = taps(k, first, number, range(3))
        raw[k, rows(first + 1, number), :] = value
        return moments(value)

    def finish(k, first, dy):
        value = raw[k, rows(first + 1, 1), :] + taps(k, first, 1, (dy,))
        raw[k, rows(first + 1, 1), :] = value
        return moments(value)

    def stat_copy(k, stage, distance):
        return pltpu.make_async_remote_copy(
            src_ref=stats[stage].at[k],
            dst_ref=peers[stage].at[k, distance - 1],
            send_sem=stat_send.at[k, stage],
            recv_sem=stat_recv.at[k, stage],
            device_id=peer_of[PLAN[stage]](distance),
            device_id_type=MESH,
        )

    def spread_stat(k, stage):
        others = peers[stage].shape[1]
        if others <= UNROLL:
            for distance in range(1, others + 1):
                stat_copy(k, stage, distance).start()
        else:
            pl.loop(1, others + 1)(lambda distance: stat_copy(k, stage, distance).start())

    def send_stat(k, chunks):
        total = sum(chunk[0] for chunk in chunks)
        centre = total / cells
        squares = sum(
            chunk[1] + jnp.square(chunk[0] / chunk[2] - centre) * chunk[2] for chunk in chunks
        )
        stats[0][k] = jnp.concatenate([total, squares], axis=0)
        spread_stat(k, 0)

    def take_stat(k):
        size = cells
        for stage in range(len(PLAN)):
            buffer = peers[stage]
            others = buffer.shape[1]
            own = stats[stage][k]
            pltpu.make_async_copy(buffer.at[k], buffer.at[k], stat_recv.at[k, stage]).wait()
            every = buffer[k]
            total = jnp.sum(every, axis=0) + own
            even = total[0:1] / (others + 1)
            gaps = jnp.sum(jnp.square(every[:, 0, :] - even), axis=0, keepdims=True)
            gaps += jnp.square(own[0:1] - even)
            squares = total[1:2] + gaps / size
            size *= others + 1
            if stage + 1 < len(PLAN):
                stats[stage + 1][k] = jnp.concatenate([total[0:1], squares], axis=0)
                spread_stat(k, stage + 1)
        average = total[0:1] / size
        scale = lax.rsqrt(squares / size + epsilon) * gain_ref[pl.ds(k, 1), :]
        return average, scale, bias_ref[pl.ds(k, 1), :]

    def normed(k, row, norm):
        average, scale, shift = norm
        return (raw[k, span(row), :] - average) * scale + shift

    rim_first = [(0, 2), (height - 2, 2)]
    middle = [(first, 2) for first in range(2, height - 2, 2)]
    inside = [(first, 2) for first in range(1, height - 1, 2)]

    loads[0].wait()
    loads[1].wait()
    project(0)
    loads[2].wait()
    project(height - 1)
    pl.semaphore_wait(barrier, count - 1)
    send_halo(feat, 0)
    loads[3].wait()

    @pl.loop(1, height - 1, unroll=ROWS)
    def _(row):
        project(row)

    def feature_rim(row):
        put(row, jnp.maximum(feat[span(row), :].astype(F32), 0.0))

    weights[0].wait()
    chunks = [conv(0, first, number) for first, number in inside]
    raw[0, rows(1, 1), :] = taps(0, 0, 1, (1, 2))
    raw[0, rows(height, 1), :] = taps(0, height - 1, 1, (0, 1))
    take_halo(feat, 0, lambda: feature_rim(0), lambda: feature_rim(height + 1))
    chunks += [finish(0, 0, 0), finish(0, height - 1, 2)]
    send_halo(raw.at[0], 1)
    send_stat(0, chunks)

    def later_conv(k):
        weights[k].wait()
        chunks = [conv(k, first, number) for first, number in rim_first]
        if k < 3:
            send_halo(raw.at[k], k + 1)
        chunks += [conv(k, first, number) for first, number in middle]
        send_stat(k, chunks)

    def hidden(k):
        norm = take_stat(k)

        def one(row):
            put(row, jnp.maximum(normed(k, row, norm), 0.0))

        pl.loop(1, height + 1, unroll=ROWS)(one)
        take_halo(raw.at[k], k + 1, lambda: one(0), lambda: one(height + 1))

    hidden(0)
    later_conv(1)

    norm_1 = take_stat(1)

    def join(row, local):
        value = (feat[span(row), :].astype(F32) + normed(1, row, norm_1)).astype(BF16)
        if local:
            joined[span(row - 1), :] = value
        put(row, jnp.maximum(value.astype(F32), 0.0))

    pl.loop(1, height + 1, unroll=ROWS)(lambda row: join(row, True))
    take_halo(raw.at[1], 2, lambda: join(0, False), lambda: join(height + 1, False))
    later_conv(2)
    hidden(2)
    later_conv(3)
    norm_3 = take_stat(3)

    @pl.loop(0, height, unroll=ROWS)
    def _(row):
        value = joined[span(row), :].astype(F32) + normed(3, row + 1, norm_3)
        out_ref[span(row), :] = value.astype(BF16)

    end_halo(feat, 0)
    for k in range(3):
        end_halo(raw.at[k], k + 1)
    for k in range(4):
        for stage, buffer in enumerate(peers):
            pltpu.make_async_copy(buffer.at[k], buffer.at[k], stat_send.at[k, stage]).wait()


def solution(mesh):
    imgs, strips = mesh.shape["img"], mesh.shape["row"]

    def on_device(tokens, proj_weight, proj_bias, conv_weight, bn_gain, bn_bias):
        images, height, cols, embed = tokens.shape
        convs, taps, _, width, _ = conv_weight.shape
        assert images == 1 and height % 2 == 0 and height >= 4
        count = imgs * strips
        sizes = {"flat": count, "row": strips, "img": imgs, "core": 2, "chip": count // 2}
        cells = height * cols
        any_space = pl.BlockSpec(memory_space=pltpu.HBM)
        vmem = pl.BlockSpec(memory_space=pltpu.VMEM)
        out = pl.pallas_call(
            functools.partial(kernel, imgs, strips, height, cols),
            out_shape=jax.ShapeDtypeStruct((cells, width), BF16),
            in_specs=[any_space, any_space, vmem, any_space, vmem, vmem],
            out_specs=vmem,
            scratch_shapes=[
                pltpu.VMEM((cells, embed), BF16),
                pltpu.VMEM((embed, width), BF16),
                pltpu.VMEM((convs * taps, taps * width, width), BF16),
                pltpu.VMEM((cells + 2 * cols, width), BF16),
                pltpu.VMEM((cells, width), BF16),
                pltpu.VMEM((cells + 2 * cols, taps * width), BF16),
                pltpu.VMEM((convs, cells + 2 * cols, width), F32),
                [pltpu.VMEM((convs, 2, width), F32) for _ in PLAN],
                [pltpu.VMEM((convs, sizes[part] - 1, 2, width), F32) for part in PLAN],
                pltpu.SemaphoreType.DMA((4,)),
                pltpu.SemaphoreType.DMA((convs,)),
                pltpu.SemaphoreType.DMA((convs, 2)),
                pltpu.SemaphoreType.DMA((convs, 2)),
                pltpu.SemaphoreType.DMA((convs, len(PLAN))),
                pltpu.SemaphoreType.DMA((convs, len(PLAN))),
            ],
            compiler_params=pltpu.CompilerParams(
                collective_id=0, has_side_effects=True, vmem_limit_bytes=VMEM_LIMIT
            ),
        )(
            tokens.reshape(cells, embed),
            proj_weight,
            proj_bias.reshape(1, width),
            conv_weight.reshape(convs * taps, taps * width, width),
            bn_gain,
            bn_bias,
        )
        return out.reshape(images, height, cols, width)

    in_specs = (P("img", "row", None, None), P(), P(), P(), P(), P())
    return jax.shard_map(
        on_device,
        mesh=mesh,
        in_specs=in_specs,
        out_specs=P("img", "row", None, None),
        check_vma=False,
    )
```
